32 devices in a mesh: section: 2 (over y), dp: 8 (over z, core), vocab: 2 (over x).
Axes of the slice: x: 2, y: 2, z: 4, core: 2. Of those that a mesh axis runs over, the one named last changes fastest.
Arguments:
- activations: bfloat16 [2, 1024, 2048], P('section', 'dp'), may hold values from -32 to 32
- token_ids: int32 [2, 1024], replicated, may hold values from 0 to 8191
- embed_table: bfloat16 [8192, 2048], P(('dp', 'vocab')), may hold values from -3 to 3
Outputs:
- tied_grad: bfloat16 [16, 2, 256, 2048], P(('dp', 'vocab'), 'section')
The draws below stay inside these ranges and needn't reach their ends.
All inputs are finite; a program needn't handle non-finite values.
Results may differ from the reference program's by a relative error of at most 0.0029.
Values may be sent and summed in bfloat16 or wider, within the bound.
A program may use at most 128 MiB of HBM per device.

```python
import math
import jax
import jax.numpy as jnp
import numpy as np
from jax import lax

D = 2048
VOCAB_DEV = 512
TOKENS = 1024
VOCAB = 8192
N_SECTION = 2


def table_rows(key, row_numbers):
    base_key = jax.random.fold_in(key, 101)

    def one_row(row_index):
        values = jax.random.normal(jax.random.fold_in(base_key, row_index), (D,), jnp.float32)
        return jnp.clip(values * (4.0 / math.sqrt(D)), -3.0, 3.0)
    return jax.vmap(one_row)(row_numbers)


def draw_embed_table(key, part):
    return table_rows(key, jnp.arange(VOCAB, dtype=jnp.int32)).astype(jnp.bfloat16)


def draw_activations(key, part):
    draw_key = jax.random.fold_in(key, 202)
    values = jax.random.normal(draw_key, (N_SECTION, TOKENS, D), jnp.float32)
    return jnp.clip(values, -32.0, 32.0).astype(jnp.bfloat16)


def plant(entries, stream_key, smallest, largest):
    spot = [jax.random.randint(jax.random.fold_in(stream_key, axis), (), 0, length) for axis, length in enumerate(entries.shape)]
    widest = entries.shape.index(max(entries.shape))
    beside = spot[:widest] + [(spot[widest] + 1) % entries.shape[widest]] + spot[widest + 1:]
    return entries.at[tuple(spot)].set(smallest).at[tuple(beside)].set(largest)


def rank_table(number_of, lean):
    portions = [(1 << 20) // math.isqrt(standing ** lean) + 1 for standing in range(1, number_of + 1)]
    scale = 1 + sum(portions) // (1 << 30)
    return np.cumsum(np.array([max(1, weight // scale) for weight in portions]))


def ranked(stream_key, shape, count, slope):
    listing = rank_table(count, slope)
    pick = jax.random.randint(jax.random.fold_in(stream_key, 1), shape, 0, int(listing[count - 1]))
    grade = jnp.searchsorted(jnp.asarray(listing, jnp.int32), pick, side="right")
    return jax.random.permutation(jax.random.fold_in(stream_key, 2), count)[grade].astype(jnp.int32)


def setup_inputs(seed: int = 0) -> dict:
    arg_keys = jax.random.split(jax.random.key(seed), 4)
    return {
        "activations": draw_activations(jax.random.fold_in(arg_keys[3], 71), 0),
        "token_ids": plant(ranked(arg_keys[1], (N_SECTION, TOKENS), VOCAB, 1), jax.random.fold_in(arg_keys[1], 3), 0, VOCAB - 1).astype(jnp.int32),
        "embed_table": draw_embed_table(jax.random.fold_in(arg_keys[3], 71), 0),
    }


def reference(activations, token_ids, embed_table):
    cotangent = activations[0]
    hidden = activations[1]
    input_ids = token_ids[0]
    target_ids = token_ids[1]
    blocks = embed_table.shape[0] // VOCAB_DEV
    table_blocks = embed_table.reshape(blocks, VOCAB_DEV, D)
    offsets = jnp.arange(blocks, dtype=jnp.int32) * VOCAB_DEV
    columns = jnp.arange(VOCAB_DEV, dtype=jnp.int32)

    def scores(table_slab):
        return jnp.dot(hidden, table_slab.T, preferred_element_type=jnp.float32)

    def running(state_pair, table_slab):
        row_peak, row_total = state_pair
        logits = scores(table_slab)
        new_peak = jnp.maximum(row_peak, jnp.max(logits, axis=1))
        row_total = row_total * jnp.exp(row_peak - new_peak) + jnp.sum(jnp.exp(logits - new_peak[:, None]), axis=1)
        return (new_peak, row_total), None

    initial = (jnp.full((TOKENS,), -1e30, jnp.float32), jnp.zeros((TOKENS,), jnp.float32))
    (row_peak, row_total), _ = lax.scan(running, initial, table_blocks)

    def block_gradient(block_pair):
        table_slab, offset = block_pair
        logits = scores(table_slab)
        target_hot = (target_ids[:, None] == offset + columns[None, :]).astype(jnp.float32)
        input_hot = (input_ids[:, None] == offset + columns[None, :]).astype(jnp.bfloat16)
        last_section = (jnp.exp(logits - row_peak[:, None]) / row_total[:, None] - target_hot).astype(jnp.bfloat16)
        gradient = jnp.dot(last_section.T, hidden, preferred_element_type=jnp.float32)
        gradient = gradient + jnp.dot(input_hot.T, cotangent, preferred_element_type=jnp.float32)
        return gradient.astype(jnp.bfloat16)

    gradients = lax.map(block_gradient, (table_blocks, offsets))
    return gradients.reshape(blocks, N_SECTION, VOCAB_DEV // N_SECTION, D)
```

```python
import functools

import jax
import jax.numpy as jnp
from jax import lax
from jax.experimental import pallas as pl
from jax.experimental.pallas import tpu as pltpu
from jax.sharding import PartitionSpec as P

MESH = pl.DeviceIdType.MESH
NT = (((1,), (1,)), ((), ()))


def kernel(sizes, ids_ref, act_ref, table_ref, out_ref, gathered, table, logits, col_stats,
           group_stats, chain_stats, load_sem, send_sem, recv_sem, stat_send, stat_recv,
           chain_send, chain_recv):
    n_dp, n_vocab, rows, tile = sizes
    n_z = n_dp // 2
    half = rows // 2
    s = lax.axis_index("section")
    d = lax.axis_index("dp")
    v = lax.axis_index("vocab")
    z = d // 2
    c = d % 2
    h = v % 2
    other = 1 - s
    pair = v + 1 - 2 * h
    table_rows = table.shape[0]
    half_rows = table_rows // 2
    targets = {
        "left": (s, d - 2, v),
        "right": (s, d + 2, v),
        "x": (s, d, pair),
        "y": (other, d, v),
        "sib": (s, d + 1 - 2 * c, v),
    }
    lane = {"left": 0, "right": 1, "x": 2, "y": 3, "sib": 4}

    own_load = pltpu.make_async_copy(
        act_ref.at[0], gathered.at[s, pl.ds(pl.multiple_of(d * rows, rows), rows)], load_sem.at[0]
    )
    own_load.start()
    table_load = pltpu.make_async_copy(table_ref, table, load_sem.at[1])
    table_load.start()

    barrier = pltpu.get_barrier_semaphore()

    def greet(sec, dp, voc):
        pl.semaphore_signal(barrier, inc=1, device_id=(sec, dp, voc), device_id_type=MESH)

    for sec in range(2):
        for core in range(2):
            for voc in range(n_vocab):
                is_me = (sec == s) & (core == c) & (voc == v)

                @pl.when(jnp.logical_not(is_me))
                def _():
                    greet(sec, z * 2 + core, voc)
        for zz in range(n_z):
            @pl.when(zz != z)
            def _():
                greet(sec, zz * 2 + c, v)
    pl.semaphore_wait(barrier, 4 * n_vocab - 1 + 2 * (n_z - 1))

    def piece(sec, dp, k):
        first = pl.multiple_of(dp * rows + k * half, half)
        return gathered.at[sec, pl.ds(first, half)]

    def copy(to, sec, dp, k):
        where = piece(sec, dp, k)
        return pltpu.make_async_remote_copy(
            src_ref=where, dst_ref=where,
            send_sem=send_sem.at[lane[to], sec, dp // 2, k],
            recv_sem=recv_sem.at[sec, dp, k],
            device_id=targets[to], device_id_type=MESH,
        )

    def need(to, own, zz, k):
        far = jnp.abs(zz - z) >= 2
        if to == "sib":
            return jnp.bool_(True)
        if own:
            if to == "right":
                return (zz <= z) & (z < n_z - 1) & ((zz == z) | (k == h))
            if to == "left":
                return (zz >= z) & (z > 0) & ((zz == z) | (k == h))
            if to == "x":
                return far & (k == h)
            return (zz == z) | (k == h)
        if to == "x":
            return (zz != z) & (k == h)
        return jnp.bool_(False)

    order_own = ("right", "left", "y", "x", "sib")
    order_other = ("x", "sib")

    def emit(own, zz, k):
        for to in order_own if own else order_other:
            @pl.when(need(to, own, zz, k))
            def _():
                copy(to, s if own else other, zz * 2 + c, k).start()

    def arrive(sec, dp, k):
        copy("sib", sec, dp, k).wait_recv()

    def score(dp):
        tokens = gathered.at[1, pl.ds(pl.multiple_of(dp * rows, rows), rows)]
        lanes = pl.ds(pl.multiple_of(dp * rows, rows), rows)

        @pl.when(s == 1)
        def _():
            scores = lax.dot_general(table[...], tokens[...], NT, preferred_element_type=jnp.float32)
            logits[:, lanes] = scores[half_rows:]
            peak = jnp.max(scores, axis=0, keepdims=True)
            total = jnp.sum(jnp.exp(scores - peak), axis=0, keepdims=True)
            col_stats[0:1, lanes] = peak
            col_stats[1:2, lanes] = total

        @pl.when(s == 0)
        def _():
            logits[:, lanes] = lax.dot_general(
                table[:half_rows], tokens[...], NT, preferred_element_type=jnp.float32
            )

    own_load.wait()
    emit(True, z, h)
    emit(True, z, 1 - h)
    table_load.wait()

    def others(delta, act):
        for zz in (z - delta, z + delta) if delta else (z,):
            @pl.when((zz >= 0) & (zz < n_z))
            def _():
                act(zz)

    def take(own, k_own):
        def act(zz):
            arrive(s if own else other, zz * 2 + c, k_own)
            emit(own, zz, k_own)
        return act

    for step in range(1, n_z + 2):
        if step < n_z:
            others(step, take(True, h))
        if step == 1:
            others(0, take(False, h))
            others(1, take(True, 1 - h))
            others(0, take(False, 1 - h))
        if 1 <= step - 1 < n_z:
            others(step - 1, take(False, h))
        if 2 <= step - 1 < n_z:
            others(step - 1, take(True, 1 - h))
        if 1 <= step - 2 < n_z:
            others(step - 2, take(False, 1 - h))

    def sibling(sec):
        def act(zz, carry):
            for k in range(2):
                arrive(sec, zz * 2 + 1 - c, k)
            return carry
        lax.fori_loop(0, n_z, act, 0)

    sibling(1)

    def score_all(dp, carry):
        score(dp)
        return carry

    lax.fori_loop(0, n_dp, score_all, 0)

    def combine(load, count):
        peak = load(0)[0:1]
        for i in range(1, count):
            peak = jnp.maximum(peak, load(i)[0:1])
        total = jnp.zeros_like(peak)
        for i in range(count):
            both = load(i)
            total = total + both[1:2] * jnp.exp(both[0:1] - peak)
        return peak, total

    n_group = 2 * n_vocab
    mine = c * n_vocab + v

    def group_copy(slot, target_core, target_voc):
        return pltpu.make_async_remote_copy(
            src_ref=group_stats.at[mine], dst_ref=group_stats.at[mine],
            send_sem=stat_send.at[slot], recv_sem=stat_recv.at[mine],
            device_id=(s, z * 2 + target_core, target_voc), device_id_type=MESH,
        )

    def chain_copy(sec, zz):
        return pltpu.make_async_remote_copy(
            src_ref=chain_stats.at[z], dst_ref=chain_stats.at[z],
            send_sem=chain_send.at[sec, zz], recv_sem=chain_recv.at[z],
            device_id=(sec, zz * 2 + c, v), device_id_type=MESH,
        )

    def landed(buffer, sems, slot):
        pltpu.make_async_copy(buffer.at[slot], buffer.at[slot], sems.at[slot]).wait()

    @pl.when(s == 1)
    def _():
        group_stats[mine] = col_stats[...]
        for slot in range(n_group):
            @pl.when(slot != mine)
            def _():
                group_copy(slot, slot // n_vocab, slot % n_vocab).start()
        for slot in range(n_group):
            @pl.when(slot != mine)
            def _():
                landed(group_stats, stat_recv, slot)
        peak, total = combine(lambda i: group_stats[i], n_group)
        chain_stats[z, 0:1] = peak
        chain_stats[z, 1:2] = total
        for zz in range(n_z):
            for sec in range(2):
                @pl.when((sec == 0) | (zz != z))
                def _():
                    chain_copy(sec, zz).start()
        for slot in range(n_group):
            @pl.when(slot != mine)
            def _():
                group_copy(slot, slot // n_vocab, slot % n_vocab).wait_send()

    for zz in range(n_z):
        @pl.when((s == 0) | (zz != z))
        def _():
            landed(chain_stats, chain_recv, zz)
    peak, total = combine(lambda i: chain_stats[i], n_z)

    first = (d * n_vocab + v) * table_rows + s * half_rows
    row = lax.broadcasted_iota(jnp.int32, logits.shape, 0) + first
    probs = jnp.exp(logits[...] - peak) * (1.0 / total)
    last = (probs - (ids_ref[1:2, :] == row).astype(jnp.float32)).astype(jnp.bfloat16)
    first_hot = (ids_ref[0:1, :] == row).astype(jnp.float32).astype(jnp.bfloat16)

    sibling(0)
    width = out_ref.shape[1]
    for at in range(0, width, tile):
        summed = jnp.dot(last, gathered[1, :, at:at + tile], preferred_element_type=jnp.float32)
        summed = summed + jnp.dot(
            first_hot, gathered[0, :, at:at + tile], preferred_element_type=jnp.float32
        )
        out_ref[:, at:at + tile] = summed.astype(jnp.bfloat16)

    @pl.when(s == 1)
    def _():
        for zz in range(n_z):
            for sec in range(2):
                @pl.when((sec == 0) | (zz != z))
                def _():
                    chain_copy(sec, zz).wait_send()

    def drain(zz, carry):
        for k in range(2):
            for own in (True, False):
                for to in order_own if own else order_other:
                    @pl.when(need(to, own, zz, k))
                    def _():
                        copy(to, s if own else other, zz * 2 + c, k).wait_send()
        return carry

    lax.fori_loop(0, n_z, drain, 0)


def solution(mesh):
    n_dp, n_vocab = mesh.shape["dp"], mesh.shape["vocab"]

    def body(activations, token_ids, embed_table):
        _, rows, width = activations.shape
        table_rows = embed_table.shape[0]
        tokens = rows * n_dp
        half_rows = table_rows // 2
        n_z = n_dp // 2
        dma = pltpu.SemaphoreType.DMA
        grad = pl.pallas_call(
            functools.partial(kernel, (n_dp, n_vocab, rows, min(512, width))),
            out_shape=jax.ShapeDtypeStruct((half_rows, width), jnp.bfloat16),
            in_specs=[
                pl.BlockSpec(memory_space=pltpu.VMEM),
                pl.BlockSpec(memory_space=pl.ANY),
                pl.BlockSpec(memory_space=pl.ANY),
            ],
            out_specs=pl.BlockSpec(memory_space=pltpu.VMEM),
            scratch_shapes=[
                pltpu.VMEM((2, tokens, width), jnp.bfloat16),
                pltpu.VMEM((table_rows, width), jnp.bfloat16),
                pltpu.VMEM((half_rows, tokens), jnp.float32),
                pltpu.VMEM((2, tokens), jnp.float32),
                pltpu.VMEM((2 * n_vocab, 2, tokens), jnp.float32),
                pltpu.VMEM((n_z, 2, tokens), jnp.float32),
                dma((2,)),
                dma((5, 2, n_z, 2)),
                dma((2, n_dp, 2)),
                dma((2 * n_vocab,)),
                dma((2 * n_vocab,)),
                dma((2, n_z)),
                dma((n_z,)),
            ],
            compiler_params=pltpu.CompilerParams(
                collective_id=0, has_side_effects=True, vmem_limit_bytes=60 * 1024 * 1024
            ),
        )(token_ids, activations, embed_table)
        return grad.reshape(1, 1, half_rows, width)

    return jax.shard_map(
        body,
        mesh=mesh,
        in_specs=(P("section", "dp", None), P(), P(("dp", "vocab"), None)),
        out_specs=P(("dp", "vocab"), "section", None, None),
        check_vma=False,
    )
```

```python
import functools

import jax
import jax.numpy as jnp
from jax import lax
from jax.experimental import pallas as pl
from jax.experimental.pallas import tpu as pltpu
from jax.sharding import PartitionSpec as P

MESH = pl.DeviceIdType.MESH
PARTS = 4
NT = (((1,), (1,)), ((), ()))


def kernel(sizes, ids_ref, act_ref, table_ref, out_ref, gathered, table, logits, col_stats,
           group_stats, chain_stats, load_sem, send_sem, recv_sem, stat_send, stat_recv,
           chain_send, chain_recv):
    n_dp, n_vocab, rows, parts, tile = sizes
    n_z = n_dp // 2
    half = rows // 2
    part = half // parts
    s = lax.axis_index("section")
    d = lax.axis_index("dp")
    v = lax.axis_index("vocab")
    z = d // 2
    c = d % 2
    h = v % 2
    other = 1 - s
    pair = v + 1 - 2 * h
    table_rows = table.shape[0]
    half_rows = table_rows // 2
    targets = {
        "left": (s, d - 2, v),
        "right": (s, d + 2, v),
        "x": (s, d, pair),
        "y": (other, d, v),
        "sib": (s, d + 1 - 2 * c, v),
    }
    lane = {"left": 0, "right": 1, "x": 2, "y": 3, "sib": 4}

    own_load = pltpu.make_async_copy(
        act_ref.at[0], gathered.at[s, pl.ds(pl.multiple_of(d * rows, rows), rows)], load_sem.at[0]
    )
    own_load.start()
    table_load = pltpu.make_async_copy(table_ref, table, load_sem.at[1])
    table_load.start()

    barrier = pltpu.get_barrier_semaphore()

    def greet(sec, dp, voc):
        pl.semaphore_signal(barrier, inc=1, device_id=(sec, dp, voc), device_id_type=MESH)

    for sec in range(2):
        for core in range(2):
            for voc in range(n_vocab):
                is_me = (sec == s) & (core == c) & (voc == v)

                @pl.when(jnp.logical_not(is_me))
                def _():
                    greet(sec, z * 2 + core, voc)
        for zz in range(n_z):
            @pl.when(zz != z)
            def _():
                greet(sec, zz * 2 + c, v)
    pl.semaphore_wait(barrier, 4 * n_vocab - 1 + 2 * (n_z - 1))

    def piece(sec, dp, k, j):
        first = pl.multiple_of(dp * rows + k * half + j * part, part)
        return gathered.at[sec, pl.ds(first, part)]

    def copy(to, sec, dp, k, j):
        where = piece(sec, dp, k, j)
        return pltpu.make_async_remote_copy(
            src_ref=where, dst_ref=where,
            send_sem=send_sem.at[lane[to], sec, dp // 2, k, j],
            recv_sem=recv_sem.at[sec, dp, k, j],
            device_id=targets[to], device_id_type=MESH,
        )

    twin = z + 1 - 2 * (z % 2)

    def need(to, own, zz, k):
        if to == "sib":
            return jnp.bool_(True)
        if own:
            if to == "right":
                return (zz <= z) & (z < n_z - 1) & ((zz == z) | (k == h))
            if to == "left":
                return (zz >= z) & (z > 0) & ((zz == z) | (k == h))
            if to == "x":
                return (jnp.abs(zz - z) >= 2) & (k == h)
            return (zz == twin) | (k == h)
        if to == "x":
            return (zz != twin) & (k == h)
        return jnp.bool_(False)

    order_own = ("right", "left", "y", "x", "sib")
    order_other = ("x", "sib")

    def emit(own, zz, k, j, lanes):
        for to in lanes:
            @pl.when(need(to, own, zz, k))
            def _():
                copy(to, s if own else other, zz * 2 + c, k, j).start()

    def arrive(sec, dp, k, j):
        copy("sib", sec, dp, k, j).wait_recv()

    def event(own, zz, k, j):
        arrive(s if own else other, zz * 2 + c, k, j)
        emit(own, zz, k, j, order_own if own else order_other)

    def each_part(act):
        def one(j, carry):
            act(j)
            return carry
        lax.fori_loop(0, parts, one, 0)

    def from_y(index):
        near = jnp.minimum(z, n_z - 1 - z)
        paired = index < 2 * near * parts
        inside = index % (2 * parts)
        delta = index // (2 * parts) + 1
        side = 2 * (inside % 2) - 1
        rest = index - 2 * near * parts
        far_side = jnp.where(z < n_z - 1 - z, 1, -1)
        zz = jnp.where(paired, z + side * delta, z + far_side * (near + 1 + rest // parts))
        return zz, jnp.where(paired, inside // 2, rest % parts)

    def own_second_half(to):
        each_part(lambda j: copy(to, s, d, 1 - h, j).start())

    def score(dp):
        tokens = gathered.at[1, pl.ds(pl.multiple_of(dp * rows, rows), rows)]
        lanes = pl.ds(pl.multiple_of(dp * rows, rows), rows)

        @pl.when(s == 1)
        def _():
            scores = lax.dot_general(table[...], tokens[...], NT, preferred_element_type=jnp.float32)
            logits[:, lanes] = scores[half_rows:]
            peak = jnp.max(scores, axis=0, keepdims=True)
            total = jnp.sum(jnp.exp(scores - peak), axis=0, keepdims=True)
            col_stats[0:1, lanes] = peak
            col_stats[1:2, lanes] = total

        @pl.when(s == 0)
        def _():
            logits[:, lanes] = lax.dot_general(
                table[:half_rows], tokens[...], NT, preferred_element_type=jnp.float32
            )

    def score_all():
        def one(dp, carry):
            score(dp)
            return carry
        lax.fori_loop(0, n_dp, one, 0)

    def sibling(sec):
        def act(zz, carry):
            for k in range(2):
                each_part(lambda j: arrive(sec, zz * 2 + 1 - c, k, j))
            return carry
        lax.fori_loop(0, n_z, act, 0)

    def on_both_sides(delta, act):
        for zz in (z - delta, z + delta):
            @pl.when((zz >= 0) & (zz < n_z))
            def _():
                act(zz)

    own_load.wait()
    each_part(lambda j: emit(True, z, h, j, ("right", "left", "y")))
    each_part(lambda j: emit(True, z, h, j, ("sib",)))
    each_part(lambda j: emit(True, z, 1 - h, j, ("sib",)))
    pl.when((z > 0) & (z == n_z - 1))(lambda: own_second_half("left"))
    pl.when((z == 0) & (z < n_z - 1))(lambda: own_second_half("right"))

    def slot(t):
        def links(j):
            if t + 1 < n_z:
                on_both_sides(t + 1, lambda zz: event(True, zz, h, j))
            if t == 0:
                event(False, z, h, j)
            elif t < n_z:
                zz, jj = from_y((t - 1) * parts + j)
                event(False, zz, h, jj)

        if t < n_z:
            each_part(links)
        if t < n_z - 1:
            pl.when((z > 0) & (t == n_z - 2 - z))(lambda: own_second_half("left"))
            pl.when((z < n_z - 1) & (t == z - 1))(lambda: own_second_half("right"))

        def second(j):
            if 1 <= t < n_z:
                pl.when((z > 0) & (t == z))(lambda: event(True, z - 1, 1 - h, j))
                pl.when((z < n_z - 1) & (t == n_z - 1 - z))(
                    lambda: event(True, z + 1, 1 - h, j)
                )
            if t == 1:
                event(False, z, 1 - h, j)
            if 2 <= t < n_z:
                on_both_sides(t, lambda zz: event(True, zz, 1 - h, j))
            if t == n_z:
                event(False, twin, 1 - h, j)
            if 3 <= t:
                zz, jj = from_y((t - 3) * parts + j)
                pl.when(zz != twin)(lambda: event(False, zz, 1 - h, jj))

        if t >= 1:
            each_part(second)

    for t in range(n_z):
        slot(t)
        if t == 0:
            table_load.wait()

    def combine(load, count):
        peak = load(0)[0:1]
        for i in range(1, count):
            peak = jnp.maximum(peak, load(i)[0:1])
        total = jnp.zeros_like(peak)
        for i in range(count):
            both = load(i)
            total = total + both[1:2] * jnp.exp(both[0:1] - peak)
        return peak, total

    n_group = 2 * n_vocab
    mine = c * n_vocab + v

    def group_copy(slot, target_core, target_voc):
        return pltpu.make_async_remote_copy(
            src_ref=group_stats.at[mine], dst_ref=group_stats.at[mine],
            send_sem=stat_send.at[slot], recv_sem=stat_recv.at[mine],
            device_id=(s, z * 2 + target_core, target_voc), device_id_type=MESH,
        )

    def chain_copy(sec, zz):
        return pltpu.make_async_remote_copy(
            src_ref=chain_stats.at[z], dst_ref=chain_stats.at[z],
            send_sem=chain_send.at[sec, zz], recv_sem=chain_recv.at[z],
            device_id=(sec, zz * 2 + c, v), device_id_type=MESH,
        )

    def landed(buffer, sems, slot):
        pltpu.make_async_copy(buffer.at[slot], buffer.at[slot], sems.at[slot]).wait()

    @pl.when(s == 1)
    def _():
        sibling(1)
        score_all()
        group_stats[mine] = col_stats[...]
        for at in range(n_group):
            @pl.when(at != mine)
            def _():
                group_copy(at, at // n_vocab, at % n_vocab).start()

    slot(n_z)

    @pl.when(s == 1)
    def _():
        for at in range(n_group):
            @pl.when(at != mine)
            def _():
                landed(group_stats, stat_recv, at)
        peak, total = combine(lambda i: group_stats[i], n_group)
        chain_stats[z, 0:1] = peak
        chain_stats[z, 1:2] = total
        for zz in range(n_z):
            for sec in range(2):
                @pl.when((sec == 0) | (zz != z))
                def _():
                    chain_copy(sec, zz).start()
        for at in range(n_group):
            @pl.when(at != mine)
            def _():
                group_copy(at, at // n_vocab, at % n_vocab).wait_send()

    slot(n_z + 1)

    @pl.when(s == 0)
    def _():
        sibling(1)
        score_all()

    for zz in range(n_z):
        @pl.when((s == 0) | (zz != z))
        def _():
            landed(chain_stats, chain_recv, zz)
    peak, total = combine(lambda i: chain_stats[i], n_z)

    first = (d * n_vocab + v) * table_rows + s * half_rows
    row = lax.broadcasted_iota(jnp.int32, logits.shape, 0) + first
    probs = jnp.exp(logits[...] - peak) * (1.0 / total)
    last = (probs - (ids_ref[1:2, :] == row).astype(jnp.float32)).astype(jnp.bfloat16)
    first_hot = (ids_ref[0:1, :] == row).astype(jnp.float32).astype(jnp.bfloat16)

    sibling(0)
    width = out_ref.shape[1]
    for at in range(0, width, tile):
        summed = jnp.dot(last, gathered[1, :, at:at + tile], preferred_element_type=jnp.float32)
        summed = summed + jnp.dot(
            first_hot, gathered[0, :, at:at + tile], preferred_element_type=jnp.float32
        )
        out_ref[:, at:at + tile] = summed.astype(jnp.bfloat16)

    @pl.when(s == 1)
    def _():
        for zz in range(n_z):
            for sec in range(2):
                @pl.when((sec == 0) | (zz != z))
                def _():
                    chain_copy(sec, zz).wait_send()

    def drain(zz, carry):
        for k in range(2):
            for own in (True, False):
                for to in order_own if own else order_other:
                    @pl.when(need(to, own, zz, k))
                    def _():
                        sec = s if own else other
                        each_part(lambda j: copy(to, sec, zz * 2 + c, k, j).wait_send())
        return carry

    lax.fori_loop(0, n_z, drain, 0)


def solution(mesh):
    n_dp, n_vocab = mesh.shape["dp"], mesh.shape["vocab"]

    def body(activations, token_ids, embed_table):
        _, rows, width = activations.shape
        table_rows = embed_table.shape[0]
        tokens = rows * n_dp
        half_rows = table_rows // 2
        n_z = n_dp // 2
        dma = pltpu.SemaphoreType.DMA
        grad = pl.pallas_call(
            functools.partial(kernel, (n_dp, n_vocab, rows, PARTS, min(512, width))),
            out_shape=jax.ShapeDtypeStruct((half_rows, width), jnp.bfloat16),
            in_specs=[
                pl.BlockSpec(memory_space=pltpu.VMEM),
                pl.BlockSpec(memory_space=pl.ANY),
                pl.BlockSpec(memory_space=pl.ANY),
            ],
            out_specs=pl.BlockSpec(memory_space=pltpu.VMEM),
            scratch_shapes=[
                pltpu.VMEM((2, tokens, width), jnp.bfloat16),
                pltpu.VMEM((table_rows, width), jnp.bfloat16),
                pltpu.VMEM((half_rows, tokens), jnp.float32),
                pltpu.VMEM((2, tokens), jnp.float32),
                pltpu.VMEM((2 * n_vocab, 2, tokens), jnp.float32),
                pltpu.VMEM((n_z, 2, tokens), jnp.float32),
                dma((2,)),
                dma((5, 2, n_z, 2, PARTS)),
                dma((2, n_dp, 2, PARTS)),
                dma((2 * n_vocab,)),
                dma((2 * n_vocab,)),
                dma((2, n_z)),
                dma((n_z,)),
            ],
            compiler_params=pltpu.CompilerParams(
                collective_id=0, has_side_effects=True, vmem_limit_bytes=60 * 1024 * 1024
            ),
        )(token_ids, activations, embed_table)
        return grad.reshape(1, 1, half_rows, width)

    return jax.shard_map(
        body,
        mesh=mesh,
        in_specs=(P("section", "dp", None), P(), P(("dp", "vocab"), None)),
        out_specs=P(("dp", "vocab"), "section", None, None),
        check_vma=False,
    )
```

```python
import functools

import jax
import jax.numpy as jnp
from jax import lax
from jax.experimental import pallas as pl
from jax.experimental.pallas import tpu as pltpu
from jax.sharding import PartitionSpec as P

MESH = pl.DeviceIdType.MESH
PARTS = 4
NT = (((1,), (1,)), ((), ()))


def kernel(sizes, ids_ref, act_ref, table_ref, out_ref, gathered, table, logits, col_stats,
           group_stats, chain_stats, load_sem, send_sem, recv_sem, stat_send, stat_recv,
           chain_send, chain_recv):
    n_dp, n_vocab, rows, parts, tile = sizes
    n_z = n_dp // 2
    half = rows // 2
    part = half // parts
    s = lax.axis_index("section")
    d = lax.axis_index("dp")
    v = lax.axis_index("vocab")
    z = d // 2
    c = d % 2
    h = v % 2
    other = 1 - s
    pair = v + 1 - 2 * h
    table_rows = table.shape[0]
    half_rows = table_rows // 2
    targets = {
        "left": (s, d - 2, v),
        "right": (s, d + 2, v),
        "x": (s, d, pair),
        "y": (other, d, v),
        "sib": (s, d + 1 - 2 * c, v),
    }
    lane = {"left": 0, "right": 1, "x": 2, "y": 3, "sib": 4}

    own_load = pltpu.make_async_copy(
        act_ref.at[0], gathered.at[s, pl.ds(pl.multiple_of(d * rows, rows), rows)], load_sem.at[0]
    )
    own_load.start()
    table_load = pltpu.make_async_copy(table_ref, table, load_sem.at[1])
    table_load.start()

    barrier = pltpu.get_barrier_semaphore()

    def greet(sec, dp, voc):
        pl.semaphore_signal(barrier, inc=1, device_id=(sec, dp, voc), device_id_type=MESH)

    for sec in range(2):
        for core in range(2):
            for voc in range(n_vocab):
                is_me = (sec == s) & (core == c) & (voc == v)

                @pl.when(jnp.logical_not(is_me))
                def _():
                    greet(sec, z * 2 + core, voc)
        for zz in range(n_z):
            @pl.when(zz != z)
            def _():
                greet(sec, zz * 2 + c, v)
    pl.semaphore_wait(barrier, 4 * n_vocab - 1 + 2 * (n_z - 1))

    def piece(sec, zz, k, j, core=None):
        core = c if core is None else core
        first = (zz * 2 + core) * rows + k * half + (0 if j is None else j * part)
        size = half if j is None else part
        return gathered.at[sec, pl.ds(pl.multiple_of(first, size), size)]

    def copy(to, sec, zz, k, j, core=None):
        where = piece(sec, zz, k, j, core)
        dp = zz * 2 + (c if core is None else core)
        return pltpu.make_async_remote_copy(
            src_ref=where, dst_ref=where,
            send_sem=send_sem.at[lane[to], sec, zz, k],
            recv_sem=recv_sem.at[sec, dp, k, 0 if j is None or to == "x" else j],
            device_id=targets[to], device_id_type=MESH,
        )

    twin = z + 1 - 2 * (z % 2)

    def need(to, own, zz, k):
        if to == "sib":
            return jnp.bool_(True)
        if own:
            if to == "right":
                return (zz <= z) & (z < n_z - 1) & ((zz == z) | (k == h))
            if to == "left":
                return (zz >= z) & (z > 0) & ((zz == z) | (k == h))
            if to == "x":
                return (jnp.abs(zz - z) >= 2) & (k == h)
            return (zz == twin) | (k == h)
        if to == "x":
            return (zz != twin) & (k == h)
        return jnp.bool_(False)

    order_own = ("right", "left", "y", "x", "sib")
    order_other = ("x", "sib")

    def emit(own, zz, k, j, lanes):
        for to in lanes:
            @pl.when(need(to, own, zz, k))
            def _():
                copy(to, s if own else other, zz, k, j).start()

    def relay(own, zz, j):
        sec = s if own else other
        copy("sib", sec, zz, h, j).wait_recv()
        emit(own, zz, h, j, order_own[:-1] if own else order_other[:-1])
        if j == parts - 1:
            copy("sib", sec, zz, h, None).start()

    def settle(own, zz):
        sec = s if own else other
        copy("sib", sec, zz, 1 - h, None).wait_recv()
        if own:
            emit(own, zz, 1 - h, None, ("y",))
        copy("sib", sec, zz, 1 - h, None).start()

    near = jnp.minimum(z, n_z - 1 - z)
    far_side = jnp.where(z < n_z - 1 - z, 1, -1)

    def from_y(t, j):
        index = (t - 1) * parts + j
        delta = index // (2 * parts) + 1
        inside = index % (2 * parts)
        paired = delta <= near
        zz = jnp.where(
            paired, z + (2 * (inside % 2) - 1) * delta,
            z + far_side * (near + 1 + index // parts - 2 * near),
        )
        return zz, jnp.where(paired, inside // 2, index % parts)

    def y_shard(t):
        delta = (t + 1) // 2
        paired = z + (delta if t % 2 == 0 else -delta)
        return jnp.where(delta <= near, paired, z + far_side * (t - near))

    def own_second_half(to):
        copy(to, s, z, 1 - h, None).start()

    def score(dp):
        tokens = gathered.at[1, pl.ds(pl.multiple_of(dp * rows, rows), rows)]
        lanes = pl.ds(pl.multiple_of(dp * rows, rows), rows)

        @pl.when(s == 1)
        def _():
            scores = lax.dot_general(table[...], tokens[...], NT, preferred_element_type=jnp.float32)
            logits[:, lanes] = scores[half_rows:]
            peak = jnp.max(scores, axis=0, keepdims=True)
            total = jnp.sum(jnp.exp(scores - peak), axis=0, keepdims=True)
            col_stats[0:1, lanes] = peak
            col_stats[1:2, lanes] = total

        @pl.when(s == 0)
        def _():
            logits[:, lanes] = lax.dot_general(
                table[:half_rows], tokens[...], NT, preferred_element_type=jnp.float32
            )

    def score_all():
        def one(dp, carry):
            score(dp)
            return carry
        lax.fori_loop(0, n_dp, one, 0)

    def sibling(sec):
        for zz in range(n_z):
            for k in range(2):
                copy("sib", sec, zz, k, None, 1 - c).wait_recv()

    def on_both_sides(delta, act):
        for zz in (z - delta, z + delta):
            @pl.when((zz >= 0) & (zz < n_z))
            def _():
                act(zz)

    own_load.wait()
    for j in range(parts):
        emit(True, z, h, j, ("right", "left", "y"))
    pl.when((z > 0) & (z == n_z - 1))(lambda: own_second_half("left"))
    pl.when((z == 0) & (z < n_z - 1))(lambda: own_second_half("right"))
    emit(True, z, h, None, ("sib",))
    emit(True, z, 1 - h, None, ("sib",))

    def slot(t):
        for j in range(parts if t < n_z else 0):
            if t + 1 < n_z:
                on_both_sides(t + 1, lambda zz: relay(True, zz, j))
            if t == 0:
                relay(False, z, j)
            else:
                zz, jj = from_y(t, j)
                relay_y(zz, jj, j)
        if t < n_z - 1:
            pl.when((z > 0) & (t == n_z - 2 - z))(lambda: own_second_half("left"))
            pl.when((z < n_z - 1) & (t == z - 1))(lambda: own_second_half("right"))
        if 1 <= t < n_z:
            pl.when((z > 0) & (t == z))(lambda: settle(True, z - 1))
            pl.when((z < n_z - 1) & (t == n_z - 1 - z))(lambda: settle(True, z + 1))
        if t == 1:
            settle(False, z)
        if 2 <= t < n_z:
            on_both_sides(t, lambda zz: settle(True, zz))
        if t == n_z:
            settle(False, twin)
        if 3 <= t:
            zz = y_shard(t - 2)
            pl.when(zz != twin)(lambda: settle(False, zz))

    def relay_y(zz, jj, j):
        copy("sib", other, zz, h, jj).wait_recv()
        emit(False, zz, h, jj, ("x",))

        @pl.when(jj == parts - 1)
        def _():
            copy("sib", other, zz, h, None).start()

    for t in range(n_z):
        slot(t)
        if t == 0:
            table_load.wait()

    def combine(load, count):
        peak = load(0)[0:1]
        for i in range(1, count):
            peak = jnp.maximum(peak, load(i)[0:1])
        total = jnp.zeros_like(peak)
        for i in range(count):
            both = load(i)
            total = total + both[1:2] * jnp.exp(both[0:1] - peak)
        return peak, total

    n_group = 2 * n_vocab
    mine = c * n_vocab + v

    def group_copy(slot, target_core, target_voc):
        return pltpu.make_async_remote_copy(
            src_ref=group_stats.at[mine], dst_ref=group_stats.at[mine],
            send_sem=stat_send.at[slot], recv_sem=stat_recv.at[mine],
            device_id=(s, z * 2 + target_core, target_voc), device_id_type=MESH,
        )

    def chain_copy(sec, zz):
        return pltpu.make_async_remote_copy(
            src_ref=chain_stats.at[z], dst_ref=chain_stats.at[z],
            send_sem=chain_send.at[sec, zz], recv_sem=chain_recv.at[z],
            device_id=(sec, zz * 2 + c, v), device_id_type=MESH,
        )

    def landed(buffer, sems, slot):
        pltpu.make_async_copy(buffer.at[slot], buffer.at[slot], sems.at[slot]).wait()

    @pl.when(s == 1)
    def _():
        sibling(1)
        score_all()
        group_stats[mine] = col_stats[...]
        for at in range(n_group):
            @pl.when(at != mine)
            def _():
                group_copy(at, at // n_vocab, at % n_vocab).start()

    slot(n_z)

    @pl.when(s == 1)
    def _():
        for at in range(n_group):
            @pl.when(at != mine)
            def _():
                landed(group_stats, stat_recv, at)
        peak, total = combine(lambda i: group_stats[i], n_group)
        chain_stats[z, 0:1] = peak
        chain_stats[z, 1:2] = total
        for zz in range(n_z):
            for sec in range(2):
                @pl.when((sec == 0) | (zz != z))
                def _():
                    chain_copy(sec, zz).start()
        for at in range(n_group):
            @pl.when(at != mine)
            def _():
                group_copy(at, at // n_vocab, at % n_vocab).wait_send()

    slot(n_z + 1)

    @pl.when(s == 0)
    def _():
        sibling(1)
        score_all()

    for zz in range(n_z):
        @pl.when((s == 0) | (zz != z))
        def _():
            landed(chain_stats, chain_recv, zz)
    peak, total = combine(lambda i: chain_stats[i], n_z)

    first = (d * n_vocab + v) * table_rows + s * half_rows
    row = lax.broadcasted_iota(jnp.int32, logits.shape, 0) + first
    probs = jnp.exp(logits[...] - peak) * (1.0 / total)
    last = (probs - (ids_ref[1:2, :] == row).astype(jnp.float32)).astype(jnp.bfloat16)
    first_hot = (ids_ref[0:1, :] == row).astype(jnp.float32).astype(jnp.bfloat16)

    sibling(0)
    width = out_ref.shape[1]
    for at in range(0, width, tile):
        summed = jnp.dot(last, gathered[1, :, at:at + tile], preferred_element_type=jnp.float32)
        summed = summed + jnp.dot(
            first_hot, gathered[0, :, at:at + tile], preferred_element_type=jnp.float32
        )
        out_ref[:, at:at + tile] = summed.astype(jnp.bfloat16)

    @pl.when(s == 1)
    def _():
        for zz in range(n_z):
            for sec in range(2):
                @pl.when((sec == 0) | (zz != z))
                def _():
                    chain_copy(sec, zz).wait_send()

    for zz in range(n_z):
        for k in (h, 1 - h):
            for own in (True, False):
                for to in order_own if own else order_other:
                    @pl.when(need(to, own, zz, k))
                    def _():
                        copy(to, s if own else other, zz, k, None).wait_send()


def solution(mesh):
    n_dp, n_vocab = mesh.shape["dp"], mesh.shape["vocab"]

    def body(activations, token_ids, embed_table):
        _, rows, width = activations.shape
        table_rows = embed_table.shape[0]
        tokens = rows * n_dp
        half_rows = table_rows // 2
        n_z = n_dp // 2
        dma = pltpu.SemaphoreType.DMA
        grad = pl.pallas_call(
            functools.partial(kernel, (n_dp, n_vocab, rows, PARTS, min(512, width))),
            out_shape=jax.ShapeDtypeStruct((half_rows, width), jnp.bfloat16),
            in_specs=[
                pl.BlockSpec(memory_space=pltpu.VMEM),
                pl.BlockSpec(memory_space=pl.ANY),
                pl.BlockSpec(memory_space=pl.ANY),
            ],
            out_specs=pl.BlockSpec(memory_space=pltpu.VMEM),
            scratch_shapes=[
                pltpu.VMEM((2, tokens, width), jnp.bfloat16),
                pltpu.VMEM((table_rows, width), jnp.bfloat16),
                pltpu.VMEM((half_rows, tokens), jnp.float32),
                pltpu.VMEM((2, tokens), jnp.float32),
                pltpu.VMEM((2 * n_vocab, 2, tokens), jnp.float32),
                pltpu.VMEM((n_z, 2, tokens), jnp.float32),
                dma((2,)),
                dma((5, 2, n_z, 2)),
                dma((2, n_dp, 2, PARTS)),
                dma((2 * n_vocab,)),
                dma((2 * n_vocab,)),
                dma((2, n_z)),
                dma((n_z,)),
            ],
            compiler_params=pltpu.CompilerParams(
                collective_id=0, has_side_effects=True, vmem_limit_bytes=60 * 1024 * 1024
            ),
        )(token_ids, activations, embed_table)
        return grad.reshape(1, 1, half_rows, width)

    return jax.shard_map(
        body,
        mesh=mesh,
        in_specs=(P("section", "dp", None), P(), P(("dp", "vocab"), None)),
        out_specs=P(("dp", "vocab"), "section", None, None),
        check_vma=False,
    )
```

```python
import functools

import jax
import jax.numpy as jnp
from jax import lax
from jax.experimental import pallas as pl
from jax.experimental.pallas import tpu as pltpu
from jax.sharding import PartitionSpec as P

MESH = pl.DeviceIdType.MESH
PARTS = 4
VMEM_MIB = 60
NT = (((1,), (1,)), ((), ()))


def kernel(sizes, ids_ref, act_ref, table_ref, out_ref, gathered, table, logits, col_stats,
           group_stats, chain_stats, load_sem, send_sem, recv_sem, stat_send, stat_recv,
           chain_send, chain_recv):
    n_dp, n_vocab, rows, parts, tile = sizes
    n_z = n_dp // 2
    half = rows // 2
    part = half // parts
    s = lax.axis_index("section")
    d = lax.axis_index("dp")
    v = lax.axis_index("vocab")
    z = d // 2
    c = d % 2
    h = v % 2
    other = 1 - s
    pair = v + 1 - 2 * h
    table_rows = table.shape[0]
    half_rows = table_rows // 2
    targets = {
        "left": (s, d - 2, v),
        "right": (s, d + 2, v),
        "x": (s, d, pair),
        "y": (other, d, v),
        "sib": (s, d + 1 - 2 * c, v),
    }
    lane = {"left": 0, "right": 1, "x": 2, "y": 3, "sib": 4}

    own_load = pltpu.make_async_copy(
        act_ref.at[0], gathered.at[s, pl.ds(pl.multiple_of(d * rows, rows), rows)], load_sem.at[0]
    )
    own_load.start()
    table_load = pltpu.make_async_copy(table_ref, table, load_sem.at[1])
    table_load.start()

    barrier = pltpu.get_barrier_semaphore()

    def greet(sec, dp, voc):
        pl.semaphore_signal(barrier, inc=1, device_id=(sec, dp, voc), device_id_type=MESH)

    for sec in range(2):
        for core in range(2):
            for voc in range(n_vocab):
                is_me = (sec == s) & (core == c) & (voc == v)

                @pl.when(jnp.logical_not(is_me))
                def _():
                    greet(sec, z * 2 + core, voc)
        for zz in range(n_z):
            @pl.when(zz != z)
            def _():
                greet(sec, zz * 2 + c, v)
    pl.semaphore_wait(barrier, 4 * n_vocab - 1 + 2 * (n_z - 1))

    def piece(sec, zz, k, j, core=None):
        core = c if core is None else core
        first = (zz * 2 + core) * rows + k * half + (0 if j is None else j * part)
        size = half if j is None else part
        return gathered.at[sec, pl.ds(pl.multiple_of(first, size), size)]

    def copy(to, sec, zz, k, j, core=None):
        where = piece(sec, zz, k, j, core)
        dp = zz * 2 + (c if core is None else core)
        return pltpu.make_async_remote_copy(
            src_ref=where, dst_ref=where,
            send_sem=send_sem.at[lane[to], sec, zz, k],
            recv_sem=recv_sem.at[sec, dp, k, 0 if j is None or to == "x" else j],
            device_id=targets[to], device_id_type=MESH,
        )

    twin = z + 1 - 2 * (z % 2)

    def need(to, own, zz, k):
        if to == "sib":
            return jnp.bool_(True)
        if own:
            if to == "right":
                return (zz <= z) & (z < n_z - 1) & ((zz == z) | (k == h))
            if to == "left":
                return (zz >= z) & (z > 0) & ((zz == z) | (k == h))
            if to == "x":
                return (jnp.abs(zz - z) >= 2) & (k == h)
            return (zz == twin) | (k == h)
        if to == "x":
            return (zz != twin) & (k == h)
        return jnp.bool_(False)

    order_own = ("right", "left", "y", "x", "sib")
    order_other = ("x", "sib")

    def emit(own, zz, k, j, lanes):
        for to in lanes:
            @pl.when(need(to, own, zz, k))
            def _():
                copy(to, s if own else other, zz, k, j).start()

    def relay(own, zz, j):
        sec = s if own else other
        copy("sib", sec, zz, h, j).wait_recv()
        emit(own, zz, h, j, order_own[:-1] if own else order_other[:-1])
        if j == parts - 1:
            copy("sib", sec, zz, h, None).start()

    def settle(own, zz):
        sec = s if own else other
        copy("sib", sec, zz, 1 - h, None).wait_recv()
        if own:
            emit(own, zz, 1 - h, None, ("y",))
        copy("sib", sec, zz, 1 - h, None).start()

    near = jnp.minimum(z, n_z - 1 - z)
    far_side = jnp.where(z < n_z - 1 - z, 1, -1)

    def from_y(t, j):
        index = (t - 1) * parts + j
        delta = index // (2 * parts) + 1
        inside = index % (2 * parts)
        paired = delta <= near
        zz = jnp.where(
            paired, z + (2 * (inside % 2) - 1) * delta,
            z + far_side * (near + 1 + index // parts - 2 * near),
        )
        return zz, jnp.where(paired, inside // 2, index % parts)

    def y_shard(t):
        delta = (t + 1) // 2
        paired = z + (delta if t % 2 == 0 else -delta)
        return jnp.where(delta <= near, paired, z + far_side * (t - near))

    def own_second_half(to):
        copy(to, s, z, 1 - h, None).start()

    def score(dp):
        tokens = gathered.at[1, pl.ds(pl.multiple_of(dp * rows, rows), rows)]
        lanes = pl.ds(pl.multiple_of(dp * rows, rows), rows)

        @pl.when(s == 1)
        def _():
            scores = lax.dot_general(table[...], tokens[...], NT, preferred_element_type=jnp.float32)
            logits[:, lanes] = scores[half_rows:]
            peak = jnp.max(scores, axis=0, keepdims=True)
            total = jnp.sum(jnp.exp(scores - peak), axis=0, keepdims=True)
            col_stats[0:1, lanes] = peak
            col_stats[1:2, lanes] = total

        @pl.when(s == 0)
        def _():
            logits[:, lanes] = lax.dot_general(
                table[:half_rows], tokens[...], NT, preferred_element_type=jnp.float32
            )

    def score_all():
        def one(dp, carry):
            score(dp)
            return carry
        lax.fori_loop(0, n_dp, one, 0)

    def sibling_shard(sec, zz):
        for k in range(2):
            copy("sib", sec, zz, k, None, 1 - c).wait_recv()

    def sibling(sec):
        for zz in range(n_z):
            sibling_shard(sec, zz)

    def early_score(zz):
        sibling_shard(1, zz)
        score(zz * 2)
        score(zz * 2 + 1)

    def on_both_sides(delta, act):
        for zz in (z - delta, z + delta):
            @pl.when((zz >= 0) & (zz < n_z))
            def _():
                act(zz)

    own_load.wait()
    for j in range(parts):
        emit(True, z, h, j, ("right", "left", "y"))
    pl.when((z > 0) & (z == n_z - 1))(lambda: own_second_half("left"))
    pl.when((z == 0) & (z < n_z - 1))(lambda: own_second_half("right"))
    emit(True, z, h, None, ("sib",))
    emit(True, z, 1 - h, None, ("sib",))

    def slot(t):
        for j in range(parts if t < n_z else 0):
            if t + 1 < n_z:
                on_both_sides(t + 1, lambda zz: relay(True, zz, j))
            if t == 0:
                relay(False, z, j)
            else:
                zz, jj = from_y(t, j)
                relay_y(zz, jj, j)
        if t < n_z - 1:
            pl.when((z > 0) & (t == n_z - 2 - z))(lambda: own_second_half("left"))
            pl.when((z < n_z - 1) & (t == z - 1))(lambda: own_second_half("right"))
        if 1 <= t < n_z:
            pl.when((z > 0) & (t == z))(lambda: settle(True, z - 1))
            pl.when((z < n_z - 1) & (t == n_z - 1 - z))(lambda: settle(True, z + 1))
        if t == 1:
            settle(False, z)
        if 2 <= t < n_z:
            on_both_sides(t, lambda zz: settle(True, zz))
        if t == n_z:
            settle(False, twin)
        if 3 <= t:
            zz = y_shard(t - 2)
            pl.when(zz != twin)(lambda: settle(False, zz))

    def relay_y(zz, jj, j):
        copy("sib", other, zz, h, jj).wait_recv()
        emit(False, zz, h, jj, ("x",))

        @pl.when(jj == parts - 1)
        def _():
            copy("sib", other, zz, h, None).start()

    for t in range(n_z):
        slot(t)
        if t == 0:
            table_load.wait()
        else:
            @pl.when(s == 1)
            def _():
                if t == 1:
                    early_score(z)
                else:
                    on_both_sides(t, early_score)

    def combine(load, count):
        peak = load(0)[0:1]
        for i in range(1, count):
            peak = jnp.maximum(peak, load(i)[0:1])
        total = jnp.zeros_like(peak)
        for i in range(count):
            both = load(i)
            total = total + both[1:2] * jnp.exp(both[0:1] - peak)
        return peak, total

    n_group = 2 * n_vocab
    mine = c * n_vocab + v

    def group_copy(slot, target_core, target_voc):
        return pltpu.make_async_remote_copy(
            src_ref=group_stats.at[mine], dst_ref=group_stats.at[mine],
            send_sem=stat_send.at[slot], recv_sem=stat_recv.at[mine],
            device_id=(s, z * 2 + target_core, target_voc), device_id_type=MESH,
        )

    def chain_copy(sec, zz):
        return pltpu.make_async_remote_copy(
            src_ref=chain_stats.at[z], dst_ref=chain_stats.at[z],
            send_sem=chain_send.at[sec, zz], recv_sem=chain_recv.at[z],
            device_id=(sec, zz * 2 + c, v), device_id_type=MESH,
        )

    def landed(buffer, sems, slot):
        pltpu.make_async_copy(buffer.at[slot], buffer.at[slot], sems.at[slot]).wait()

    @pl.when(s == 1)
    def _():
        on_both_sides(1, early_score)
        group_stats[mine] = col_stats[...]
        for at in range(n_group):
            @pl.when(at != mine)
            def _():
                group_copy(at, at // n_vocab, at % n_vocab).start()

    slot(n_z)

    @pl.when(s == 1)
    def _():
        for at in range(n_group):
            @pl.when(at != mine)
            def _():
                landed(group_stats, stat_recv, at)
        peak, total = combine(lambda i: group_stats[i], n_group)
        chain_stats[z, 0:1] = peak
        chain_stats[z, 1:2] = total
        for zz in range(n_z):
            for sec in range(2):
                @pl.when((sec == 0) | (zz != z))
                def _():
                    chain_copy(sec, zz).start()
        for at in range(n_group):
            @pl.when(at != mine)
            def _():
                group_copy(at, at // n_vocab, at % n_vocab).wait_send()

    slot(n_z + 1)

    @pl.when(s == 0)
    def _():
        sibling(1)
        score_all()

    for zz in range(n_z):
        @pl.when((s == 0) | (zz != z))
        def _():
            landed(chain_stats, chain_recv, zz)
    peak, total = combine(lambda i: chain_stats[i], n_z)

    first = (d * n_vocab + v) * table_rows + s * half_rows
    row = lax.broadcasted_iota(jnp.int32, logits.shape, 0) + first
    probs = jnp.exp(logits[...] - peak) * (1.0 / total)
    last = (probs - (ids_ref[1:2, :] == row).astype(jnp.float32)).astype(jnp.bfloat16)
    first_hot = (ids_ref[0:1, :] == row).astype(jnp.float32).astype(jnp.bfloat16)

    sibling(0)
    width = out_ref.shape[1]
    for at in range(0, width, tile):
        summed = jnp.dot(last, gathered[1, :, at:at + tile], preferred_element_type=jnp.float32)
        summed = summed + jnp.dot(
            first_hot, gathered[0, :, at:at + tile], preferred_element_type=jnp.float32
        )
        out_ref[:, at:at + tile] = summed.astype(jnp.bfloat16)

    @pl.when(s == 1)
    def _():
        for zz in range(n_z):
            for sec in range(2):
                @pl.when((sec == 0) | (zz != z))
                def _():
                    chain_copy(sec, zz).wait_send()

    for zz in range(n_z):
        for k in (h, 1 - h):
            for own in (True, False):
                for to in order_own if own else order_other:
                    @pl.when(need(to, own, zz, k))
                    def _():
                        copy(to, s if own else other, zz, k, None).wait_send()


def solution(mesh):
    n_dp, n_vocab = mesh.shape["dp"], mesh.shape["vocab"]

    def body(activations, token_ids, embed_table):
        _, rows, width = activations.shape
        table_rows = embed_table.shape[0]
        tokens = rows * n_dp
        half_rows = table_rows // 2
        n_z = n_dp // 2
        dma = pltpu.SemaphoreType.DMA
        grad = pl.pallas_call(
            functools.partial(kernel, (n_dp, n_vocab, rows, PARTS, min(512, width))),
            out_shape=jax.ShapeDtypeStruct((half_rows, width), jnp.bfloat16),
            in_specs=[
                pl.BlockSpec(memory_space=pltpu.VMEM),
                pl.BlockSpec(memory_space=pl.ANY),
                pl.BlockSpec(memory_space=pl.ANY),
            ],
            out_specs=pl.BlockSpec(memory_space=pltpu.VMEM),
            scratch_shapes=[
                pltpu.VMEM((2, tokens, width), jnp.bfloat16),
                pltpu.VMEM((table_rows, width), jnp.bfloat16),
                pltpu.VMEM((half_rows, tokens), jnp.float32),
                pltpu.VMEM((2, tokens), jnp.float32),
                pltpu.VMEM((2 * n_vocab, 2, tokens), jnp.float32),
                pltpu.VMEM((n_z, 2, tokens), jnp.float32),
                dma((2,)),
                dma((5, 2, n_z, 2)),
                dma((2, n_dp, 2, PARTS)),
                dma((2 * n_vocab,)),
                dma((2 * n_vocab,)),
                dma((2, n_z)),
                dma((n_z,)),
            ],
            compiler_params=pltpu.CompilerParams(
                collective_id=0, has_side_effects=True, vmem_limit_bytes=VMEM_MIB * 1024 * 1024
            ),
        )(token_ids, activations, embed_table)
        return grad.reshape(1, 1, half_rows, width)

    return jax.shard_map(
        body,
        mesh=mesh,
        in_specs=(P("section", "dp", None), P(), P(("dp", "vocab"), None)),
        out_specs=P(("dp", "vocab"), "section", None, None),
        check_vma=False,
    )
```
